256 devices in a mesh: row: 8 (over z), col: 16 (over x, y_hi, core), img: 2 (over y_lo).
Axes of the slice: x: 4, y: 4 (y_hi: 2, y_lo: 2; y = y_hi * 2 + y_lo), z: 8, core: 2. Of those that a mesh axis runs over, the one named last changes fastest.
Arguments:
- tokens: bfloat16 [192, 576, 512], P(('img', 'row'), 'col'), parts along dimension 0, may hold values from -6 to 6
- qkv_weight: bfloat16 [2, 512, 1536], P(None, 'col'), may hold values from -0.25 to 0.25
- proj_weight: bfloat16 [2, 512, 512], P(None, 'col'), may hold values from -0.25 to 0.25
- hidden_weight: bfloat16 [2, 512, 2048], P(None, 'col'), may hold values from -0.25 to 0.25
- output_weight: bfloat16 [2, 2048, 512], P(None, 'col'), may hold values from -0.125 to 0.125
- norm_gain: float32 [2, 2, 512], replicated, may hold values from 0.25 to 1.75
- model_bias: float32 [2, 4, 512], replicated, may hold values from -2 to 2
- qkv_bias: float32 [2, 1536], replicated, may hold values from -2 to 2
- hidden_bias: float32 [2, 2048], replicated, may hold values from -2 to 2
- position_bias: float32 [2, 16, 23, 23], replicated, may hold values from -3 to 250
Outputs:
- result: bfloat16 [192, 576, 512], P(('img', 'row'), 'col'), parts along dimension 0
The draws below stay inside these ranges and needn't reach their ends.
There are 2 independent parts, one for each index of `img`. The reference program is written for one: setup_inputs(seed, part) draws one part's arguments, and reference() takes and returns one part's arrays. A program takes and returns all parts, laid end to end along the dimension named above; an argument that names none is the same for every part. Nothing has to cross between parts.
All inputs are finite; a program needn't handle non-finite values.
Results may differ from the reference program's by a relative error of at most 0.012.
Values may be sent and summed in bfloat16 or wider, within the bound.
No kernel may reach another device: no remote copies, remote signals or barrier semaphores. Data moves between devices by JAX's collectives and lax.ppermute only.
A program may use at most 192 MiB of HBM per device.

```python
import jax
import jax.numpy as jnp
from jax import lax

D = 512
HEADS = 16
FF = 2048
WIN = 12
BLOCKS = 2
SHIFT = 6
H = 96
W = 576


def draw_position_bias(key, part):
    values = jnp.clip(jax.random.normal(key, (BLOCKS, HEADS, 2 * WIN - 1, 2 * WIN - 1), jnp.float32), -3.0, 3.0)
    return values


def steps_of(key, shape, cuts, smallest, largest):
    loudness = 1.0
    for dim, shards_of in cuts:
        heights = jax.random.uniform(jax.random.fold_in(jax.random.fold_in(key, 6), dim), (shards_of,), jnp.float32, smallest / len(cuts), largest / len(cuts))
        loudness = loudness * jnp.repeat(jnp.exp(heights), shape[dim] // shards_of).reshape((-1,) + (1,) * (len(shape) - 1 - dim))
    return loudness


def bell_draw(stream_key, extent, scale, limit, cuts=(), kind=jnp.bfloat16):
    drawn = scale * jax.random.normal(stream_key, extent, jnp.float32)
    if cuts:
        drawn = drawn * steps_of(stream_key, extent, cuts, -0.22, 0.18)
    return jnp.clip(drawn, -limit, limit).astype(kind)


def setup_inputs(seed: int = 0, part: int = 0) -> dict:
    key_list = jax.random.split(jax.random.key(seed), 11)
    own_keys = jax.random.split(jax.random.fold_in(key_list[10], part), 11)
    tokens = bell_draw(own_keys[0], (H, W, D), 1.0, 6.0, ((0, 8), (1, 16)))
    qkv_weight = bell_draw(key_list[1], (BLOCKS, D, 3 * D), D ** -0.5, 0.25, ((1, 16),))
    proj_weight = bell_draw(key_list[2], (BLOCKS, D, D), D ** -0.5, 0.25, ((1, 16),))
    hidden_weight = bell_draw(key_list[3], (BLOCKS, D, FF), D ** -0.5, 0.25, ((1, 16),))
    output_weight = bell_draw(key_list[4], (BLOCKS, FF, D), FF ** -0.5, 0.125, ((1, 16),))
    norm_gain = jnp.clip(1.0 + 0.15 * jax.random.normal(key_list[5], (BLOCKS, 2, D), jnp.float32), 0.25, 1.75)
    model_bias = bell_draw(key_list[6], (BLOCKS, 4, D), 0.3, 2.0, (), jnp.float32)
    qkv_bias = bell_draw(key_list[7], (BLOCKS, 3 * D), 0.3, 2.0, (), jnp.float32)
    hidden_bias = bell_draw(key_list[8], (BLOCKS, FF), 0.3, 2.0, (), jnp.float32)
    position_bias = draw_position_bias(jax.random.fold_in(key_list[10], 71), part)
    return dict(tokens=tokens, qkv_weight=qkv_weight, proj_weight=proj_weight, hidden_weight=hidden_weight, output_weight=output_weight, norm_gain=norm_gain, model_bias=model_bias, qkv_bias=qkv_bias, hidden_bias=hidden_bias, position_bias=position_bias)


def layer_norm(values, gain, shift):
    center = values - lax.optimization_barrier(jnp.mean(values, -1, keepdims=True))
    spread = lax.optimization_barrier(jnp.mean(center * center, -1, keepdims=True))
    return center * lax.rsqrt(spread + 1e-05) * gain + shift

def bias_table(table):
    offsets = jnp.arange(WIN)
    delta = (offsets[:, None] - offsets[None, :] + WIN - 1).astype(jnp.int32)
    picked = table[:, delta[:, None, :, None], delta[None, :, None, :]]
    return picked.reshape(table.shape[0], WIN * WIN, WIN * WIN)

def labels(start, count, total):
    index = start + jnp.arange(count)
    return (index >= total - WIN).astype(jnp.int32) + (index >= total - SHIFT).astype(jnp.int32)

def window_attention(qkv_band, position, label_grid):
    width = qkv_band.shape[1]
    nwin = width // WIN
    head_dim = D // HEADS
    split = qkv_band.reshape(WIN, nwin, WIN, 3, HEADS, head_dim).transpose(1, 0, 2, 3, 4, 5)
    split = split.reshape(nwin, WIN * WIN, 3, HEADS, head_dim)
    query = split[:, :, 0].astype(jnp.float32)
    keys = split[:, :, 1].astype(jnp.float32)
    values = split[:, :, 2].astype(jnp.float32)
    scores = jnp.einsum('wqhd,wkhd->whqk', query, keys) / jnp.sqrt(jnp.float32(head_dim)) + position[None]
    if label_grid is not None:
        window_labels = label_grid.reshape(WIN, nwin, WIN).transpose(1, 0, 2).reshape(nwin, WIN * WIN)
        same = window_labels[:, :, None] == window_labels[:, None, :]
        scores = jnp.where(same[:, None], scores, -1000000000.0)
    attn = jax.nn.softmax(scores, -1).astype(jnp.bfloat16)
    heads_out = jnp.einsum('whqk,wkhd->wqhd', attn.astype(jnp.float32), values).astype(jnp.bfloat16)
    return heads_out.reshape(nwin, WIN, WIN, D).transpose(1, 0, 2, 3).reshape(WIN, width, D)

def swin_block(grid, layer, masked, qkv_weight, proj_weight, hidden_weight, output_weight, norm_gain, model_bias, qkv_bias, hidden_bias, position_bias):
    height, width = (grid.shape[0], grid.shape[1])
    flat = grid.reshape(-1, D).astype(jnp.float32)
    normed = layer_norm(flat, norm_gain[layer, 0], model_bias[layer, 0]).astype(jnp.bfloat16)
    qkv = (jnp.dot(normed, qkv_weight[layer], preferred_element_type=jnp.float32) + qkv_bias[layer]).astype(jnp.bfloat16)
    qkv = qkv.reshape(height, width, 3 * D)
    position = bias_table(position_bias[layer])
    column_labels = labels(0, width, width)

    def one_band(band):
        start = (band * WIN).astype(jnp.int32)
        rows_here = lax.dynamic_slice_in_dim(qkv, start, WIN, 0)
        if masked:
            grid_labels = labels(start, WIN, height)[:, None] * 3 + column_labels[None, :]
        else:
            grid_labels = None
        return window_attention(rows_here, position, grid_labels)
    heads_out = lax.map(one_band, jnp.arange(height // WIN).astype(jnp.int32)).reshape(-1, D)
    middle = flat + (jnp.dot(heads_out, proj_weight[layer], preferred_element_type=jnp.float32) + model_bias[layer, 2])
    normed2 = layer_norm(middle, norm_gain[layer, 1], model_bias[layer, 1]).astype(jnp.bfloat16)
    hidden = jax.nn.gelu(jnp.dot(normed2, hidden_weight[layer], preferred_element_type=jnp.float32) + hidden_bias[layer], approximate=False).astype(jnp.bfloat16)
    final = middle + (jnp.dot(hidden, output_weight[layer], preferred_element_type=jnp.float32) + model_bias[layer, 3])
    return final.astype(jnp.bfloat16).reshape(height, width, D)

def reference(tokens, qkv_weight, proj_weight, hidden_weight, output_weight, norm_gain, model_bias, qkv_bias, hidden_bias, position_bias):
    params = (qkv_weight, proj_weight, hidden_weight, output_weight, norm_gain, model_bias, qkv_bias, hidden_bias, position_bias)
    first = swin_block(tokens, 0, False, *params)
    shifted = jnp.roll(first, (-SHIFT, -SHIFT), (0, 1))
    second = swin_block(shifted, 1, True, *params)
    return jnp.roll(second, (SHIFT, SHIFT), (0, 1))
```

```python
import math

import jax
import jax.numpy as jnp
import numpy as np
from jax import lax
from jax.experimental import pallas as pl
from jax.experimental.pallas import tpu as pltpu
from jax.sharding import PartitionSpec as P


HEADS = 16
WIN = 12
SHIFT = 6
D = 512
FF = 2048
HD = 32
KEYS = WIN * WIN
NWIN = 3
TOK = KEYS * NWIN
LOG2E = math.log2(math.e)
BF = jnp.bfloat16
F32 = jnp.float32
VMEM_LIMIT = 60 * 1024 * 1024
NT = (((1,), (1,)), ((), ()))
NN = (((1,), (0,)), ((), ()))
AXES = ("row", "x", "yh", "c", "img")
SIZES = (8, 4, 2, 2, 2)


def dot(a, b, dims=NN):
    return lax.dot_general(a, b, dims, preferred_element_type=F32)


def layer_norm(values, gain, shift):
    center = values - jnp.mean(values, -1, keepdims=True)
    spread = jnp.mean(center * center, -1, keepdims=True)
    return center * lax.rsqrt(spread + 1e-05) * gain + shift


def bias_kernel(masked, t_ref, side_ref, out_ref, rows, mask):
    lane = lax.broadcasted_iota(jnp.int32, (HEADS, 128), 1)
    n_off = 2 * WIN - 1
    for cb in range(WIN):
        tiles = [jnp.zeros((HEADS, 128), F32) for _ in range(3)]
        for ro in range(n_off):
            moved = pltpu.roll(t_ref[ro], (ro * WIN - (WIN - 1 - cb)) % 128, 1)
            for tile in range(ro * WIN // 128, (ro * WIN + WIN - 1) // 128 + 1):
                low = ro * WIN - tile * 128
                tiles[tile] = jnp.where((lane >= low) & (lane < low + WIN), moved, tiles[tile])
        for tile in range(3):
            rows[tile, (cb + 4) * HEADS : (cb + 5) * HEADS, :] = tiles[tile] * LOG2E
    if masked:
        last_row = (lax.axis_index("row") == 7).astype(F32)
        col = (lax.axis_index("x") * 2 + lax.axis_index("yh")) * 2 + lax.axis_index("c")
        last_col = (col == 15).astype(F32)
        below = side_ref[0:1, :TOK]
        right = side_ref[1:2, :TOK]
        here = side_ref[2:3, :TOK]
        key_right = (lax.broadcasted_iota(jnp.int32, (WIN, 1), 0) >= SHIFT).astype(F32)
        across = last_col * here * jnp.abs(right - key_right)
        for rb in range(WIN):
            down = last_row * jnp.abs(below - (1.0 if rb >= SHIFT else 0.0))
            mask[rb * WIN : (rb + 1) * WIN, :] = jnp.maximum(across, down) * -1e9
    lane = lax.broadcasted_iota(jnp.int32, (16, 128), 1)
    upper = lax.broadcasted_iota(jnp.int32, (8, 128), 0) < 4

    def one_line(mine, at, t):
        value = None
        for w in range(NWIN):
            for s in range(3):
                low = max(KEYS * w, s * 128 + KEYS * w - at) - t * 128
                high = min(KEYS * (w + 1), (s + 1) * 128 + KEYS * w - at) - t * 128
                if max(low, 0) >= min(high, 128):
                    continue
                moved = pltpu.roll(mine[s], (KEYS * w - at) % 128, 1)
                value = moved if value is None else jnp.where(lane >= low, moved, value)
        return value

    def one_head(h, carry):
        even = [rows[tile, pl.ds(h + 4 * HEADS, 16, stride=HEADS), :] for tile in range(3)]
        odd = [rows[tile, pl.ds(h, 16, stride=HEADS), :] for tile in range(3)]
        for pair_at in range(WIN // 2):
            for t in range(4):
                first = one_line(even, (WIN - 1 - 2 * pair_at) * WIN, t)
                second = one_line(odd, (WIN - 2 - 2 * pair_at) * WIN, t)
                whole = jnp.concatenate(
                    [first[:8], jnp.where(upper, first[8:], second[:8]), second[8:]], axis=0)
                width = min(TOK - t * 128, 128)
                at = slice(pair_at * 24, (pair_at + 1) * 24), slice(t * 128, t * 128 + width)
                whole = whole[:, :width]
                if masked:
                    whole = whole + mask[at[0], at[1]]
                out_ref[h, at[0], at[1]] = whole
        return carry

    lax.fori_loop(0, HEADS, one_head, 0)


def bias_table(t, masked, after=()):
    vm = pl.BlockSpec(memory_space=pltpu.VMEM)
    at = np.arange(512)
    side = np.zeros((8, 512), np.float32)
    side[0] = at % KEYS >= SHIFT * WIN
    side[1] = at % WIN >= SHIFT
    side[2] = (at >= 2 * KEYS) & (at < TOK)

    def body(*refs):
        bias_kernel(masked, refs[0], refs[1], *refs[-3:])

    return pl.pallas_call(
        body,
        out_shape=jax.ShapeDtypeStruct((HEADS, KEYS, TOK), F32),
        in_specs=[vm, vm] + [pl.BlockSpec(memory_space=pl.ANY)] * len(after),
        out_specs=vm,
        scratch_shapes=[pltpu.VMEM((3, 20 * HEADS, 128), F32), pltpu.VMEM((KEYS, TOK), F32)],
        compiler_params=pltpu.CompilerParams(vmem_limit_bytes=VMEM_LIMIT),
        name="bias_table",
    )(t, jnp.asarray(side), *after)


def fetch_blocks(refs, tags, first, count, dst, sem, whole):
    core = lax.axis_index("c")
    my_yh = lax.axis_index("yh")
    my_x = lax.axis_index("x")
    copies = []
    for ref, (kind, flip, shift) in zip(refs, tags):
        c = 1 - core if flip else core
        for i in range(ref.shape[0]):
            if kind == "x":
                col = i * 4 + (1 - my_yh if shift else my_yh) * 2 + c
            else:
                col = lax.rem(my_x + 4 - shift, 4) * 4 + i * 2 + c
            if whole:
                to = dst.at[col]
            else:
                to = dst.at[:, pl.ds(pl.multiple_of(col * 32, 32), 32), :]
            copy = pltpu.make_async_copy(ref.at[i, pl.ds(first, count)], to, sem)
            copy.start()
            copies.append(copy)
    return copies


def attn_kernel(n_pieces, layer, tags, assemble, first, *refs):
    n_w = len(tags)
    pieces = refs[:n_pieces]
    wrefs = refs[n_pieces : n_pieces + n_w]
    (perm_ref, permt_ref, bq_all, gain_ref, mbias_ref, bt_ref, ho_ref,
     xs, qs, ks, vts, ots, bts, w_ref, sem) = refs[n_pieces + n_w :]
    bq_ref = bq_all.at[layer : layer + 1]
    weights = fetch_blocks(wrefs, tags, first, 3, w_ref, sem.at[0], False)
    fetch = pltpu.make_async_copy(bt_ref, bts, sem.at[1])
    fetch.start()
    assemble(pieces, xs)
    normed = layer_norm(xs[...], gain_ref[layer, 0:1], mbias_ref[layer, 0:1]).astype(BF)
    nw = dot(perm_ref[...], normed).astype(BF)
    for copy in weights:
        copy.wait()
    scale = LOG2E / math.sqrt(HD)
    for kind in range(2):
        y = dot(nw, w_ref[kind]) + bq_ref[:, kind * D : (kind + 1) * D]
        if kind == 0:
            y = y * scale
        dst = qs if kind == 0 else ks
        for w in range(NWIN):
            rows = slice(w * KEYS, (w + 1) * KEYS)
            for g in range(4):
                tile = y[rows, g * 128 : (g + 1) * 128]
                if w:
                    tile = pltpu.roll(tile, HD * w, 1)
                dst[rows, g * 128 : (g + 1) * 128] = tile.astype(BF)
    v = (dot(nw, w_ref[2]) + bq_ref[:, 2 * D :]).astype(BF)
    eye = (lax.broadcasted_iota(jnp.int32, (128, 128), 0)
           == lax.broadcasted_iota(jnp.int32, (128, 128), 1)).astype(BF)
    for w in range(NWIN):
        for g in range(4):
            vt = dot(eye, v[w * KEYS : (w + 1) * KEYS, g * 128 : (g + 1) * 128], NT).astype(BF)
            for hh in range(4):
                vts[g * 4 + hh, w * HD : (w + 1) * HD, :] = vt[hh * HD : (hh + 1) * HD]
    for h in range(HEADS):
        vts[h, NWIN * HD :, :] = jnp.ones((16, KEYS), BF)
    lane_slot = lax.broadcasted_iota(jnp.int32, (1, 128), 1) // HD
    slot = [(lane_slot == s).astype(F32).astype(BF) for s in range(4)]
    win = lax.broadcasted_iota(jnp.int32, (1, TOK), 1)
    fetch.wait()
    for h in range(HEADS):
        g, hh = divmod(h, 4)
        lanes = slice(g * 128, (g + 1) * 128)
        kcat = ks[0:KEYS, lanes] * slot[hh]
        for w in range(1, NWIN):
            kcat = kcat + ks[w * KEYS : (w + 1) * KEYS, lanes] * slot[(hh + w) % 4]
        qbd = jnp.concatenate(
            [qs[w * KEYS : (w + 1) * KEYS, lanes] * slot[(hh + w) % 4] for w in range(NWIN)], axis=0)
        st = dot(kcat, qbd, NT) + bts[h]
        p = jnp.exp2(st - jnp.max(st, axis=0, keepdims=True)).astype(BF)
        o = dot(vts[h], p)
        mine = jnp.where(win < KEYS, o[0:HD], jnp.where(win < 2 * KEYS, o[HD : 2 * HD], o[2 * HD : 3 * HD]))
        ots[h * HD : (h + 1) * HD, :] = (mine * (1.0 / o[3 * HD : 3 * HD + 1])).astype(BF)
    ho_ref[...] = dot(permt_ref[...], ots[...], NT).astype(BF)


def attention(layer, pieces, assemble, weights, perm, permt, bq, gain, mbias, bt):
    (blocks, tags), first = weights
    n, m = len(pieces), len(blocks)
    hbm = pl.BlockSpec(memory_space=pl.ANY)
    vm = pl.BlockSpec(memory_space=pltpu.VMEM)
    return pl.pallas_call(
        lambda *refs: attn_kernel(n, layer, tags, assemble, first, *refs),
        out_shape=jax.ShapeDtypeStruct((TOK, D), BF),
        in_specs=[vm] * n + [hbm] * m + [vm] * 5 + [hbm],
        out_specs=vm,
        scratch_shapes=[
            pltpu.VMEM((TOK, D), F32),
            pltpu.VMEM((TOK, D), BF),
            pltpu.VMEM((TOK, D), BF),
            pltpu.VMEM((HEADS, NWIN * HD + 16, KEYS), BF),
            pltpu.VMEM((D, TOK), BF),
            pltpu.VMEM((HEADS, KEYS, TOK), F32),
            pltpu.VMEM((3, D, D), BF),
            pltpu.SemaphoreType.DMA((2,)),
        ],
        compiler_params=pltpu.CompilerParams(vmem_limit_bytes=VMEM_LIMIT),
        cost_estimate=pl.CostEstimate(flops=10_000_000_000, bytes_accessed=8_000_000, transcendentals=0),
        name="attention",
    )(*pieces, *blocks, perm, permt, bq, gain, mbias, bt)


def mlp_kernel(n_pieces, layer, tags, firsts, assemble, finish, *refs):
    pieces = refs[:n_pieces]
    ho_ref, bh_all, gain_ref, mbias_ref = refs[n_pieces : n_pieces + 4]
    bh_ref = bh_all.at[layer : layer + 1]
    at = n_pieces + 4
    blocks = []
    for group in tags:
        blocks.append(refs[at : at + len(group)])
        at += len(group)
    outs = refs[at:-6]
    xs, acc, wp_ref, wh_ref, wo_ref, sem = refs[-6:]
    proj = fetch_blocks(blocks[0], tags[0], firsts[0], 1, wp_ref, sem.at[0], False)
    up = fetch_blocks(blocks[1], tags[1], firsts[1], 4, wh_ref, sem.at[1], False)
    down = fetch_blocks(blocks[2], tags[2], firsts[2], 4, wo_ref, sem.at[2], True)
    assemble(pieces, xs)
    for copy in proj:
        copy.wait()
    mid = xs[...] + (dot(ho_ref[...], wp_ref[0]) + mbias_ref[layer, 2:3])
    xs[...] = mid
    n2 = layer_norm(mid, gain_ref[layer, 1:2], mbias_ref[layer, 1:2]).astype(BF)
    step = 512
    for copy in up:
        copy.wait()
    for c in range(FF // step):
        cols = slice(c * step, (c + 1) * step)
        z = dot(n2, wh_ref[c]) + bh_ref[:, cols]
        hid = (0.5 * z * (1.0 + lax.erf(z * math.sqrt(0.5)))).astype(BF)
        if c == 0:
            for copy in down:
                copy.wait()
        part = dot(hid, wo_ref[4 * c : 4 * c + 4].reshape(step, D))
        acc[...] = part if c == 0 else acc[...] + part
    xs[...] = xs[...] + (acc[...] + mbias_ref[layer, 3:4])
    finish(xs, outs)


def mlp(layer, pieces, assemble, finish, weights, ho, bh, gain, mbias):
    outs = part_shapes()
    tags = [group[1] for group, _ in weights]
    firsts = [first for _, first in weights]
    blocks = [b for group, _ in weights for b in group[0]]
    n = len(pieces)
    vm = pl.BlockSpec(memory_space=pltpu.VMEM)
    return pl.pallas_call(
        lambda *refs: mlp_kernel(n, layer, tags, firsts, assemble, finish, *refs),
        out_shape=outs,
        in_specs=[vm] * (n + 4) + [pl.BlockSpec(memory_space=pl.ANY)] * len(blocks),
        out_specs=[vm] * len(outs),
        scratch_shapes=[
            pltpu.VMEM((TOK, D), F32),
            pltpu.VMEM((TOK, D), F32),
            pltpu.VMEM((1, D, D), BF),
            pltpu.VMEM((4, D, D), BF),
            pltpu.VMEM((16, 4, 32, D), BF),
            pltpu.SemaphoreType.DMA((3,)),
        ],
        compiler_params=pltpu.CompilerParams(vmem_limit_bytes=VMEM_LIMIT),
        cost_estimate=pl.CostEstimate(flops=10_000_000_000, bytes_accessed=8_000_000, transcendentals=0),
        name="mlp",
    )(*pieces, ho, bh, gain, mbias, *blocks)


ROWS = WIN
COLS = WIN * NWIN
KEEP = COLS - SHIFT


def assemble_plain(pieces, xs):
    for r in range(ROWS):
        xs[r * COLS : (r + 1) * COLS, :] = pieces[0][r].astype(F32)


def assemble_shifted(pieces, xs):
    own, right, below, corner = pieces
    for r in range(SHIFT):
        xs[r * COLS : r * COLS + KEEP, :] = own[r].astype(F32)
        xs[r * COLS + KEEP : (r + 1) * COLS, :] = right[r].astype(F32)
        at = (r + SHIFT) * COLS
        xs[at : at + KEEP, :] = below[r].astype(F32)
        xs[at + KEEP : at + COLS, :] = corner[r].astype(F32)


def finish_first(xs, outs):
    own, right, below, corner = outs
    for r in range(SHIFT):
        top = xs[r * COLS : (r + 1) * COLS, :].astype(BF)
        below[r] = top[SHIFT:]
        corner[r] = top[:SHIFT]
        low = xs[(r + SHIFT) * COLS : (r + SHIFT + 1) * COLS, :].astype(BF)
        own[r] = low[SHIFT:]
        right[r] = low[:SHIFT]


def finish_second(xs, outs):
    own, right, below, corner = outs
    for r in range(SHIFT):
        top = xs[r * COLS : (r + 1) * COLS, :].astype(BF)
        own[r] = top[:KEEP]
        right[r] = top[KEEP:]
        low = xs[(r + SHIFT) * COLS : (r + SHIFT + 1) * COLS, :].astype(BF)
        below[r] = low[:KEEP]
        corner[r] = low[KEEP:]


def join_kernel(own, right, below, corner, out):
    for r in range(SHIFT):
        out[r] = jnp.concatenate([corner[r].astype(F32), below[r].astype(F32)], axis=0).astype(BF)
        out[r + SHIFT] = jnp.concatenate([right[r].astype(F32), own[r].astype(F32)], axis=0).astype(BF)


def join(*pieces):
    return pl.pallas_call(
        join_kernel,
        out_shape=jax.ShapeDtypeStruct((ROWS, COLS, D), BF),
        name="join",
    )(*pieces)


def part_shapes():
    return (
        jax.ShapeDtypeStruct((SHIFT, KEEP, D), BF),
        jax.ShapeDtypeStruct((SHIFT, SHIFT, D), BF),
        jax.ShapeDtypeStruct((SHIFT, KEEP, D), BF),
        jax.ShapeDtypeStruct((SHIFT, SHIFT, D), BF),
    )


def permutations():
    perm = np.zeros((TOK, TOK), np.float32)
    for r in range(ROWS):
        for c in range(COLS):
            perm[(c // WIN) * KEYS + r * WIN + c % WIN, r * COLS + c] = 1
    return jnp.asarray(perm, BF), jnp.asarray(perm.T, BF)


def bias_rows(table):
    return jnp.pad(table.transpose(0, 2, 1, 3), ((0, 0), (0, 0), (0, 0), (0, 128 - (2 * WIN - 1))))


def send(block, where):
    pairs = []
    for at in np.ndindex(*SIZES):
        row, x, yh, c, img = at
        row2, x2, y2, c2 = where(row, x, yh * 2 + img, c)
        to = (row2 % 8, x2 % 4, y2 % 4 // 2, c2, y2 % 2)
        pairs.append((int(np.ravel_multi_index(at, SIZES)), int(np.ravel_multi_index(to, SIZES))))
    return lax.ppermute(block, AXES, pairs)


def shift_tokens(block, rows, cols):
    def where(row, x, y, c):
        col = (x * 4 + y // 2 * 2 + c + cols) % 16
        return row + rows, col // 4, col // 2 % 2 * 2 + y % 2, col % 2

    return send(block, where)


def swap_cores(block):
    return send(block, lambda row, x, y, c: (row, x, y, 1 - c))


def chunk_kernel(picks, n_after, qkv, proj, hidden, output, *refs):
    outs = refs[n_after:]
    arrays = (qkv, proj, hidden, output)
    for out, group in zip(outs, picks):
        at = 0
        for layer, which in group:
            ref = arrays[which]
            for rows in range(ref.shape[1] // 32):
                for lanes in range(ref.shape[2] // D):
                    out[at] = ref[layer, rows * 32 : (rows + 1) * 32, lanes * D : (lanes + 1) * D]
                    at += 1


def chunks(picks, weights, after=()):
    sizes = [w.shape[1] // 32 * (w.shape[2] // D) for w in weights]
    counts = [sum(sizes[which] for _, which in group) for group in picks]
    return pl.pallas_call(
        lambda *refs: chunk_kernel(picks, len(after), *refs),
        out_shape=[jax.ShapeDtypeStruct((n, 32, D), BF) for n in counts],
        in_specs=[pl.BlockSpec(memory_space=pltpu.VMEM)] * 4 + [pl.BlockSpec(memory_space=pl.ANY)] * len(after),
        name="chunks",
    )(*weights, *after)


X_MOVES = (1, 3, 2)


def join_x_kernel(n_after, own, *refs):
    came, out, sem = refs[:3], refs[3 + n_after], refs[-1]
    x = lax.axis_index("x")
    copies = []
    for k, ref in enumerate((own, *came)):
        slot = x if k == 0 else lax.rem(x + 4 - X_MOVES[k - 1], 4)
        copies.append(pltpu.make_async_copy(ref, out.at[slot], sem.at[k]))
    for copy in copies:
        copy.start()
    for copy in copies:
        copy.wait()


def join_x(own, came, after):
    hbm = pl.BlockSpec(memory_space=pl.ANY)
    return pl.pallas_call(
        lambda *refs: join_x_kernel(len(after), *refs),
        out_shape=jax.ShapeDtypeStruct((4, *own.shape), BF),
        in_specs=[pl.BlockSpec(memory_space=pltpu.VMEM)] * 4 + [hbm] * len(after),
        out_specs=hbm,
        scratch_shapes=[pltpu.SemaphoreType.DMA((4,))],
        name="join_x",
    )(own, *came, *after)


def pair_kernel(own, other, *refs):
    out, sem = refs[-2:]
    yh = lax.axis_index("yh")
    copies = [
        pltpu.make_async_copy(own, out.at[yh], sem.at[0]),
        pltpu.make_async_copy(other, out.at[1 - yh], sem.at[1]),
    ]
    for copy in copies:
        copy.start()
    for copy in copies:
        copy.wait()


def pair(own, other, after):
    hbm = pl.BlockSpec(memory_space=pl.ANY)
    return pl.pallas_call(
        pair_kernel,
        out_shape=jax.ShapeDtypeStruct((2, *own.shape), BF),
        in_specs=[pl.BlockSpec(memory_space=pltpu.VMEM)] * 2 + [hbm] * len(after),
        out_specs=hbm,
        scratch_shapes=[pltpu.SemaphoreType.DMA((2,))],
        name="pair",
    )(own, other, *after)


def along_x(block):
    return [send(block, lambda row, x, y, c, dx=dx: (row, x + dx, y, c)) for dx in X_MOVES]


def across_y(block):
    return send(block, lambda row, x, y, c: (row, x, 3 - y, c))


def spread_pair(both, came):
    blocks, tags = [], []
    for dx, block in zip((0, *X_MOVES), (both, *came)):
        blocks += [block, swap_cores(block)]
        tags += [("yh", 0, dx), ("yh", 1, dx)]
    return blocks, tags


def local(
    tokens,
    qkv_weight,
    proj_weight,
    hidden_weight,
    output_weight,
    norm_gain,
    model_bias,
    qkv_bias,
    hidden_bias,
    position_bias,
):
    weights = (qkv_weight, proj_weight, hidden_weight, output_weight)
    first, rest = chunks((((0, 0),), ((0, 1), (0, 2), (0, 3))), weights)
    rows = bias_rows(position_bias)
    first_y = across_y(first)
    rest_x = along_x(rest)
    first = pair(first, first_y, ())
    first_x = along_x(first)
    qkv0 = spread_pair(first, first_x)
    (second,) = chunks((((1, 0), (1, 1), (1, 2), (1, 3)),), weights, (first,))
    second_y = across_y(second)
    table0 = bias_table(rows[0], False, (second,))
    mine = join_x(rest, rest_x, (table0,))
    other = across_y(mine)
    second = pair(second, second_y, (mine,))
    second_x = along_x(second)
    perm, permt = permutations()

    def attn(k, pieces, assemble, blocks, table):
        params = (qkv_bias, norm_gain, model_bias, table)
        return attention(k, pieces, assemble, blocks, perm, permt, *params)

    def feed(k, pieces, assemble, finish, blocks, ho):
        return mlp(k, pieces, assemble, finish, blocks, ho, hidden_bias, norm_gain, model_bias)

    ho = attn(0, (tokens,), assemble_plain, (qkv0, 0), table0)
    table1 = bias_table(rows[1], True, (ho,))
    rest0 = (mine, swap_cores(mine), other, swap_cores(other)), (("x", 0, 0), ("x", 1, 0), ("x", 0, 1), ("x", 1, 1))
    own, right, below, corner = feed(
        0, (tokens,), assemble_plain, finish_first, ((rest0, 0), (rest0, 1), (rest0, 5)), ho
    )
    below, corner, right, table1 = lax.optimization_barrier((below, corner, right, table1))
    pieces = (
        own,
        shift_tokens(right, 0, -1),
        shift_tokens(below, -1, 0),
        shift_tokens(corner, -1, -1),
    )
    layer1 = spread_pair(second, second_x)
    ho = attn(1, pieces, assemble_shifted, (layer1, 0), table1)
    own, right, below, corner = feed(
        1, pieces, assemble_shifted, finish_second, ((layer1, 3), (layer1, 4), (layer1, 8)), ho
    )
    return join(
        own,
        shift_tokens(right, 0, 1),
        shift_tokens(below, 1, 0),
        shift_tokens(corner, 1, 1),
    )


def solution(mesh):
    fine = jax.sharding.Mesh(mesh.devices.reshape(SIZES), AXES)
    tokens = P(("img", "row"), ("x", "yh", "c"), None)
    weight = P(None, ("x", "yh", "c"), None)
    in_specs = (tokens, weight, weight, weight, weight, P(), P(), P(), P(), P())

    return jax.shard_map(local, mesh=fine, in_specs=in_specs, out_specs=tokens, check_vma=False)
```

```python
import math

import jax
import jax.numpy as jnp
import numpy as np
from jax import lax
from jax.experimental import pallas as pl
from jax.experimental.pallas import tpu as pltpu
from jax.sharding import PartitionSpec as P


HEADS = 16
WIN = 12
SHIFT = 6
D = 512
FF = 2048
HD = 32
KEYS = WIN * WIN
NWIN = 3
TOK = KEYS * NWIN
LOG2E = math.log2(math.e)
BF = jnp.bfloat16
F32 = jnp.float32
MIB = 1024 * 1024
NT = (((1,), (1,)), ((), ()))
NN = (((1,), (0,)), ((), ()))
AXES = ("row", "x", "yh", "c", "img")
SIZES = (8, 4, 2, 2, 2)


def dot(a, b, dims=NN):
    return lax.dot_general(a, b, dims, preferred_element_type=F32)


def layer_norm(values, gain, shift):
    center = values - jnp.mean(values, -1, keepdims=True)
    spread = jnp.mean(center * center, -1, keepdims=True)
    return center * lax.rsqrt(spread + 1e-05) * gain + shift


def bias_kernel(masked, t_ref, side_ref, out_ref, rows, mask):
    lane = lax.broadcasted_iota(jnp.int32, (HEADS, 128), 1)
    n_off = 2 * WIN - 1
    for cb in range(WIN):
        tiles = [jnp.zeros((HEADS, 128), F32) for _ in range(3)]
        for ro in range(n_off):
            moved = pltpu.roll(t_ref[ro], (ro * WIN - (WIN - 1 - cb)) % 128, 1)
            for tile in range(ro * WIN // 128, (ro * WIN + WIN - 1) // 128 + 1):
                low = ro * WIN - tile * 128
                tiles[tile] = jnp.where((lane >= low) & (lane < low + WIN), moved, tiles[tile])
        for tile in range(3):
            rows[tile, (cb + 4) * HEADS : (cb + 5) * HEADS, :] = tiles[tile] * LOG2E
    if masked:
        last_row = (lax.axis_index("row") == 7).astype(F32)
        col = (lax.axis_index("x") * 2 + lax.axis_index("yh")) * 2 + lax.axis_index("c")
        last_col = (col == 15).astype(F32)
        below = side_ref[0:1, :TOK]
        right = side_ref[1:2, :TOK]
        here = side_ref[2:3, :TOK]
        key_right = (lax.broadcasted_iota(jnp.int32, (WIN, 1), 0) >= SHIFT).astype(F32)
        across = last_col * here * jnp.abs(right - key_right)
        for rb in range(WIN):
            down = last_row * jnp.abs(below - (1.0 if rb >= SHIFT else 0.0))
            mask[rb * WIN : (rb + 1) * WIN, :] = jnp.maximum(across, down) * -1e9
    lane = lax.broadcasted_iota(jnp.int32, (16, 128), 1)
    upper = lax.broadcasted_iota(jnp.int32, (8, 128), 0) < 4

    def one_line(mine, at, t):
        value = None
        for w in range(NWIN):
            for s in range(3):
                low = max(KEYS * w, s * 128 + KEYS * w - at) - t * 128
                high = min(KEYS * (w + 1), (s + 1) * 128 + KEYS * w - at) - t * 128
                if max(low, 0) >= min(high, 128):
                    continue
                moved = pltpu.roll(mine[s], (KEYS * w - at) % 128, 1)
                value = moved if value is None else jnp.where(lane >= low, moved, value)
        return value

    def one_head(h, carry):
        even = [rows[tile, pl.ds(h + 4 * HEADS, 16, stride=HEADS), :] for tile in range(3)]
        odd = [rows[tile, pl.ds(h, 16, stride=HEADS), :] for tile in range(3)]
        for pair_at in range(WIN // 2):
            for t in range(4):
                first = one_line(even, (WIN - 1 - 2 * pair_at) * WIN, t)
                second = one_line(odd, (WIN - 2 - 2 * pair_at) * WIN, t)
                whole = jnp.concatenate(
                    [first[:8], jnp.where(upper, first[8:], second[:8]), second[8:]], axis=0)
                width = min(TOK - t * 128, 128)
                at = slice(pair_at * 24, (pair_at + 1) * 24), slice(t * 128, t * 128 + width)
                whole = whole[:, :width]
                if masked:
                    whole = whole + mask[at[0], at[1]]
                out_ref[h, at[0], at[1]] = whole
        return carry

    lax.fori_loop(0, HEADS, one_head, 0)


def bias_table(t, masked, after=()):
    vm = pl.BlockSpec(memory_space=pltpu.VMEM)
    at = np.arange(512)
    side = np.zeros((8, 512), np.float32)
    side[0] = at % KEYS >= SHIFT * WIN
    side[1] = at % WIN >= SHIFT
    side[2] = (at >= 2 * KEYS) & (at < TOK)

    def body(*refs):
        bias_kernel(masked, refs[0], refs[1], *refs[-3:])

    return pl.pallas_call(
        body,
        out_shape=jax.ShapeDtypeStruct((HEADS, KEYS, TOK), F32),
        in_specs=[vm, vm] + [pl.BlockSpec(memory_space=pl.ANY)] * len(after),
        out_specs=vm,
        scratch_shapes=[pltpu.VMEM((3, 20 * HEADS, 128), F32), pltpu.VMEM((KEYS, TOK), F32)],
        compiler_params=pltpu.CompilerParams(vmem_limit_bytes=8 * MIB),
        name="bias_table",
    )(t, jnp.asarray(side), *after)


def fetch_blocks(refs, tags, first, count, dst, whole):
    core = lax.axis_index("c")
    my_yh = lax.axis_index("yh")
    my_x = lax.axis_index("x")
    for ref, (kind, flip, shift) in zip(refs, tags):
        c = 1 - core if flip else core
        for i in range(ref.shape[0]):
            if kind == "x":
                col = i * 4 + (1 - my_yh if shift else my_yh) * 2 + c
            else:
                col = lax.rem(my_x + 4 - shift, 4) * 4 + i * 2 + c
            block = ref[i, first : first + count]
            if whole:
                dst[col] = block
            else:
                dst[:, pl.ds(pl.multiple_of(col * 32, 32), 32), :] = block


def one_hot(where_ref, which, start, count):
    i = lax.broadcasted_iota(jnp.int32, (count, TOK), 0) + start
    return (i == where_ref[which : which + 1, :TOK]).astype(F32).astype(BF)


def attn_kernel(n_pieces, layer, tags, assemble, first, *refs):
    n_w = len(tags)
    pieces = refs[:n_pieces]
    wrefs = refs[n_pieces : n_pieces + n_w]
    at = n_pieces + n_w
    where_ref, bq_all, gain_ref, mbias_ref, bt_ref = refs[at : at + 5]
    hos = refs[at + 5 : -6]
    xs, qs, ks, vts, ots, w_ref = refs[-6:]
    bq_ref = bq_all.at[layer : layer + 1]
    fetch_blocks(wrefs, tags, first, 3, w_ref, False)
    assemble(pieces, xs)
    normed = layer_norm(xs[...], gain_ref[layer, 0:1], mbias_ref[layer, 0:1]).astype(BF)
    nw = dot(one_hot(where_ref, 0, 0, TOK), normed).astype(BF)
    scale = LOG2E / math.sqrt(HD)
    for kind in range(2):
        y = dot(nw, w_ref[kind]) + bq_ref[:, kind * D : (kind + 1) * D]
        if kind == 0:
            y = y * scale
        dst = qs if kind == 0 else ks
        for w in range(NWIN):
            rows = slice(w * KEYS, (w + 1) * KEYS)
            for g in range(4):
                tile = y[rows, g * 128 : (g + 1) * 128]
                if w:
                    tile = pltpu.roll(tile, HD * w, 1)
                dst[g, rows, :] = tile.astype(BF)
    v = (dot(nw, w_ref[2]) + bq_ref[:, 2 * D :]).astype(BF)
    eye = (lax.broadcasted_iota(jnp.int32, (128, 128), 0)
           == lax.broadcasted_iota(jnp.int32, (128, 128), 1)).astype(BF)
    for w in range(NWIN):
        for g in range(4):
            vt = dot(eye, v[w * KEYS : (w + 1) * KEYS, g * 128 : (g + 1) * 128], NT).astype(BF)
            for hh in range(4):
                vts[g * 4 + hh, w * HD : (w + 1) * HD, :] = vt[hh * HD : (hh + 1) * HD]
    for h in range(HEADS):
        vts[h, NWIN * HD :, :] = jnp.ones((16, KEYS), BF)
    lane_slot = lax.broadcasted_iota(jnp.int32, (1, 128), 1) // HD
    slot = [(lane_slot == s).astype(F32).astype(BF) for s in range(4)]
    win = lax.broadcasted_iota(jnp.int32, (1, TOK), 1)

    def four_heads(g, carry):
        for hh in range(4):
            h = g * 4 + hh
            kcat = ks[g, 0:KEYS, :] * slot[hh]
            for w in range(1, NWIN):
                kcat = kcat + ks[g, w * KEYS : (w + 1) * KEYS, :] * slot[(hh + w) % 4]
            qbd = jnp.concatenate(
                [qs[g, w * KEYS : (w + 1) * KEYS, :] * slot[(hh + w) % 4] for w in range(NWIN)], axis=0)
            st = dot(kcat, qbd, NT) + bt_ref[h]
            p = jnp.exp2(st - jnp.max(st, axis=0, keepdims=True)).astype(BF)
            o = dot(vts[h], p)
            mine = jnp.where(win < KEYS, o[0:HD], jnp.where(win < 2 * KEYS, o[HD : 2 * HD], o[2 * HD : 3 * HD]))
            ots[h] = (mine * (1.0 / o[3 * HD : 3 * HD + 1])).astype(BF)
        return carry

    lax.fori_loop(0, HEADS // 4, four_heads, 0)
    first_token = 0
    for ho_ref in hos:
        pick = one_hot(where_ref, 1, first_token, ho_ref.shape[0])
        ho_ref[...] = dot(pick, ots[...].reshape(D, TOK), NT).astype(BF)
        first_token += ho_ref.shape[0]


def attention(layer, pieces, assemble, weights, where, counts, bq, gain, mbias, bt):
    (blocks, tags), first = weights
    n, m = len(pieces), len(blocks)
    vm = pl.BlockSpec(memory_space=pltpu.VMEM)
    return pl.pallas_call(
        lambda *refs: attn_kernel(n, layer, tags, assemble, first, *refs),
        out_shape=[jax.ShapeDtypeStruct((count, D), BF) for count in counts],
        in_specs=[vm] * (n + m + 5),
        out_specs=[vm] * len(counts),
        scratch_shapes=[
            pltpu.VMEM((TOK, D), F32),
            pltpu.VMEM((4, TOK, 128), BF),
            pltpu.VMEM((4, TOK, 128), BF),
            pltpu.VMEM((HEADS, NWIN * HD + 16, KEYS), BF),
            pltpu.VMEM((HEADS, HD, TOK), BF),
            pltpu.VMEM((3, D, D), BF),
        ],
        compiler_params=pltpu.CompilerParams(vmem_limit_bytes=20 * MIB),
        cost_estimate=pl.CostEstimate(flops=10_000_000_000, bytes_accessed=8_000_000, transcendentals=0),
        name="attention",
    )(*pieces, *blocks, where, bq, gain, mbias, bt)


def mlp_kernel(n_pieces, layer, tags, firsts, assemble, finish, *refs):
    pieces = refs[:n_pieces]
    ho_ref, bh_all, gain_ref, mbias_ref = refs[n_pieces : n_pieces + 4]
    bh_ref = bh_all.at[layer : layer + 1]
    at = n_pieces + 4
    blocks = []
    for shared, group in tags:
        if shared is not None:
            blocks.append(blocks[shared])
            continue
        blocks.append(refs[at : at + len(group)])
        at += len(group)
    tags = [group for _, group in tags]
    outs = refs[at:-5]
    xs, acc, wp_ref, wh_ref, wo_ref = refs[-5:]
    fetch_blocks(blocks[0], tags[0], firsts[0], 1, wp_ref, False)
    fetch_blocks(blocks[1], tags[1], firsts[1], 4, wh_ref, False)
    fetch_blocks(blocks[2], tags[2], firsts[2], 4, wo_ref, True)
    assemble(pieces, xs)
    mid = xs[...] + (dot(ho_ref[...], wp_ref[0]) + mbias_ref[layer, 2:3])
    xs[...] = mid
    n2 = layer_norm(mid, gain_ref[layer, 1:2], mbias_ref[layer, 1:2]).astype(BF)
    step = 512
    for c in range(FF // step):
        cols = slice(c * step, (c + 1) * step)
        z = dot(n2, wh_ref[c]) + bh_ref[:, cols]
        hid = (0.5 * z * (1.0 + lax.erf(z * math.sqrt(0.5)))).astype(BF)
        part = dot(hid, wo_ref[4 * c : 4 * c + 4].reshape(step, D))
        acc[...] = part if c == 0 else acc[...] + part
    xs[...] = xs[...] + (acc[...] + mbias_ref[layer, 3:4])
    finish(xs, outs)


def mlp(layer, pieces, assemble, finish, outs, weights, ho, bh, gain, mbias):
    tokens = ho.shape[0]
    tags, blocks = [], []
    for i, (group, _) in enumerate(weights):
        same = [j for j in range(i) if weights[j][0] is group]
        tags.append((same[0] if same else None, group[1]))
        blocks += () if same else group[0]
    firsts = [first for _, first in weights]
    n = len(pieces)
    vm = pl.BlockSpec(memory_space=pltpu.VMEM)
    return pl.pallas_call(
        lambda *refs: mlp_kernel(n, layer, tags, firsts, assemble, finish, *refs),
        out_shape=outs,
        in_specs=[vm] * (n + 4 + len(blocks)),
        out_specs=[vm] * len(outs),
        scratch_shapes=[
            pltpu.VMEM((tokens, D), F32),
            pltpu.VMEM((tokens, D), F32),
            pltpu.VMEM((1, D, D), BF),
            pltpu.VMEM((4, D, D), BF),
            pltpu.VMEM((16, 4, 32, D), BF),
        ],
        compiler_params=pltpu.CompilerParams(vmem_limit_bytes=20 * MIB),
        cost_estimate=pl.CostEstimate(flops=10_000_000_000, bytes_accessed=8_000_000, transcendentals=0),
        name="mlp",
    )(*pieces, ho, bh, gain, mbias, *blocks)


ROWS = WIN
COLS = WIN * NWIN
KEEP = COLS - SHIFT


def assemble_plain(pieces, xs):
    for r in range(ROWS):
        xs[r * COLS : (r + 1) * COLS, :] = pieces[0][r].astype(F32)


SENT = SHIFT * (COLS + SHIFT)


def assemble_sent(pieces, xs):
    right, below, corner = pieces
    for r in range(SHIFT):
        xs[r * COLS : r * COLS + KEEP, :] = below[r].astype(F32)
        xs[r * COLS + KEEP : (r + 1) * COLS, :] = corner[r].astype(F32)
        at = SHIFT * (COLS + r)
        xs[at : at + SHIFT, :] = right[r].astype(F32)


def assemble_kept(pieces, xs, base=0):
    for r in range(SHIFT):
        xs[base + r * KEEP : base + (r + 1) * KEEP, :] = pieces[0][r].astype(F32)


def assemble_shifted(pieces, xs):
    assemble_sent(pieces[1:], xs)
    assemble_kept(pieces, xs, SENT)


def finish_first(xs, outs):
    own, right, below, corner = outs
    for r in range(SHIFT):
        top = xs[r * COLS : (r + 1) * COLS, :].astype(BF)
        below[r] = top[SHIFT:]
        corner[r] = top[:SHIFT]
        low = xs[(r + SHIFT) * COLS : (r + SHIFT + 1) * COLS, :].astype(BF)
        own[r] = low[SHIFT:]
        right[r] = low[:SHIFT]


def finish_sent(xs, outs):
    right, below, corner = outs
    for r in range(SHIFT):
        low = xs[r * COLS : (r + 1) * COLS, :].astype(BF)
        below[r] = low[:KEEP]
        corner[r] = low[KEEP:]
        at = SHIFT * (COLS + r)
        right[r] = xs[at : at + SHIFT, :].astype(BF)


def finish_kept(xs, outs):
    for r in range(SHIFT):
        outs[0][r] = xs[r * KEEP : (r + 1) * KEEP, :].astype(BF)


def join_kernel(own, right, below, corner, out):
    for r in range(SHIFT):
        out[r] = jnp.concatenate([corner[r].astype(F32), below[r].astype(F32)], axis=0).astype(BF)
        out[r + SHIFT] = jnp.concatenate([right[r].astype(F32), own[r].astype(F32)], axis=0).astype(BF)


def join(*pieces):
    return pl.pallas_call(
        join_kernel,
        out_shape=jax.ShapeDtypeStruct((ROWS, COLS, D), BF),
        compiler_params=pltpu.CompilerParams(vmem_limit_bytes=4 * MIB),
        name="join",
    )(*pieces)


def part_shapes():
    return (
        jax.ShapeDtypeStruct((SHIFT, KEEP, D), BF),
        jax.ShapeDtypeStruct((SHIFT, SHIFT, D), BF),
        jax.ShapeDtypeStruct((SHIFT, KEEP, D), BF),
        jax.ShapeDtypeStruct((SHIFT, SHIFT, D), BF),
    )


def places(shifted):
    table = np.full((8, 512), -1, np.int32)
    for r in range(ROWS):
        for c in range(COLS):
            if not shifted:
                at = r * COLS + c
            elif r >= SHIFT:
                at = (r - SHIFT) * COLS + c
            elif c >= KEEP:
                at = SHIFT * (COLS + r) + c - KEEP
            else:
                at = SENT + r * KEEP + c
            place = (c // WIN) * KEYS + r * WIN + c % WIN
            table[0, at] = place
            table[1, place] = at
    return jnp.asarray(table)


def bias_rows(table):
    return jnp.pad(table.transpose(0, 2, 1, 3), ((0, 0), (0, 0), (0, 0), (0, 128 - (2 * WIN - 1))))


def send(block, where):
    pairs = []
    for at in np.ndindex(*SIZES):
        row, x, yh, c, img = at
        row2, x2, y2, c2 = where(row, x, yh * 2 + img, c)
        to = (row2 % 8, x2 % 4, y2 % 4 // 2, c2, y2 % 2)
        pairs.append((int(np.ravel_multi_index(at, SIZES)), int(np.ravel_multi_index(to, SIZES))))
    return lax.ppermute(block, AXES, pairs)


def shift_tokens(block, rows, cols):
    def where(row, x, y, c):
        col = (x * 4 + y // 2 * 2 + c + cols) % 16
        return row + rows, col // 4, col // 2 % 2 * 2 + y % 2, col % 2

    return send(block, where)


def swap_cores(block):
    return send(block, lambda row, x, y, c: (row, x, y, 1 - c))


def chunk_kernel(picks, n_in, *refs):
    arrays, outs, sem = refs[:n_in], refs[n_in:-1], refs[-1]
    copies = []
    for g, (out, group) in enumerate(zip(outs, picks)):
        at = 0
        for layer, which in group:
            ref = arrays[which]
            for rows in range(ref.shape[1] // 32):
                for lanes in range(ref.shape[2] // D):
                    part = ref.at[layer, pl.ds(rows * 32, 32), pl.ds(lanes * D, D)]
                    copies.append(pltpu.make_async_copy(part, out.at[at], sem.at[g, at]))
                    at += 1
    for copy in copies:
        copy.start()
    for copy in copies:
        copy.wait()


def chunks(picks, weights):
    sizes = [w.shape[1] // 32 * (w.shape[2] // D) for w in weights]
    counts = [sum(sizes[which] for _, which in group) for group in picks]
    return pl.pallas_call(
        lambda *refs: chunk_kernel(picks, len(weights), *refs),
        out_shape=[jax.ShapeDtypeStruct((n, 32, D), BF) for n in counts],
        in_specs=[pl.BlockSpec(memory_space=pltpu.HBM)] * len(weights),
        out_specs=[pl.BlockSpec(memory_space=pltpu.VMEM)] * len(counts),
        scratch_shapes=[pltpu.SemaphoreType.DMA((len(counts), max(counts)))],
        compiler_params=pltpu.CompilerParams(vmem_limit_bytes=8 * MIB),
        name="chunks",
    )(*weights)


X_MOVES = (1, 3, 2)


def join_x_kernel(n_after, own, *refs):
    came, out = refs[:3], refs[3 + n_after]
    x = lax.axis_index("x")
    for k, ref in enumerate((own, *came)):
        out[x if k == 0 else lax.rem(x + 4 - X_MOVES[k - 1], 4)] = ref[...]


def join_x(own, came, after):
    vm = pl.BlockSpec(memory_space=pltpu.VMEM)
    return pl.pallas_call(
        lambda *refs: join_x_kernel(len(after), *refs),
        out_shape=jax.ShapeDtypeStruct((4, *own.shape), BF),
        in_specs=[vm] * 4 + [pl.BlockSpec(memory_space=pl.ANY)] * len(after),
        out_specs=vm,
        compiler_params=pltpu.CompilerParams(vmem_limit_bytes=8 * MIB),
        name="join_x",
    )(own, *came, *after)


def pair_kernel(cuts, own, other, *refs):
    yh = lax.axis_index("yh")
    for (lo, hi), out in zip(cuts, refs[-len(cuts) :]):
        out[yh] = own[lo:hi]
        out[1 - yh] = other[lo:hi]


def pair(own, other, cuts, after):
    vm = pl.BlockSpec(memory_space=pltpu.VMEM)
    return pl.pallas_call(
        lambda *refs: pair_kernel(cuts, *refs),
        out_shape=[jax.ShapeDtypeStruct((2, hi - lo, 32, D), BF) for lo, hi in cuts],
        in_specs=[vm] * 2 + [pl.BlockSpec(memory_space=pl.ANY)] * len(after),
        out_specs=[vm] * len(cuts),
        compiler_params=pltpu.CompilerParams(vmem_limit_bytes=8 * MIB),
        name="pair",
    )(own, other, *after)


def along_x(block):
    return [send(block, lambda row, x, y, c, dx=dx: (row, x + dx, y, c)) for dx in X_MOVES]


def across_y(block):
    return send(block, lambda row, x, y, c: (row, x, 3 - y, c))


def spread_pair(both, came):
    blocks, tags = [], []
    for dx, block in zip((0, *X_MOVES), (both, *came)):
        blocks += [block, swap_cores(block)]
        tags += [("yh", 0, dx), ("yh", 1, dx)]
    return blocks, tags


def local(
    tokens,
    qkv_weight,
    proj_weight,
    hidden_weight,
    output_weight,
    norm_gain,
    model_bias,
    qkv_bias,
    hidden_bias,
    position_bias,
):
    weights = (qkv_weight, proj_weight, hidden_weight, output_weight)
    (first,) = chunks((((0, 0),),), (qkv_weight,))
    rest, second = chunks((((0, 1), (0, 2), (0, 3)), ((1, 0), (1, 1), (1, 2), (1, 3))), weights)
    rows = bias_rows(position_bias)
    first_y = across_y(first)
    second_y = across_y(second)
    rest_x = along_x(rest)
    (first,) = pair(first, first_y, ((0, 3),), ())
    first_x = along_x(first)
    qkv0 = spread_pair(first, first_x)
    attn1, mlp1 = pair(second, second_y, ((0, 4), (4, 12)), (first,))
    mine = join_x(rest, rest_x, (mlp1,))
    other = across_y(mine)
    attn1_x = along_x(attn1)
    mlp1_x = along_x(mlp1)
    table0 = bias_table(rows[0], False, (mine,))

    def attn(k, pieces, assemble, blocks, table, counts):
        params = (qkv_bias, norm_gain, model_bias, table)
        return attention(k, pieces, assemble, blocks, places(k), counts, *params)

    def feed(k, pieces, assemble, finish, outs, blocks, ho):
        return mlp(k, pieces, assemble, finish, outs, blocks, ho, hidden_bias, norm_gain, model_bias)

    def exchange(right, below, corner, way):
        corner = shift_tokens(corner, way, way)
        right = shift_tokens(right, 0, way)
        below = shift_tokens(below, way, 0)
        return right, below, corner

    (ho,) = attn(0, (tokens,), assemble_plain, (qkv0, 0), table0, (TOK,))
    rest0 = (mine, swap_cores(mine), other, swap_cores(other)), (("x", 0, 0), ("x", 1, 0), ("x", 0, 1), ("x", 1, 1))
    shapes = part_shapes()
    own, *halo = feed(
        0, (tokens,), assemble_plain, finish_first, shapes, ((rest0, 0), (rest0, 1), (rest0, 5)), ho
    )
    table1 = bias_table(rows[1], True, tuple(halo))
    pieces = (own, *exchange(*halo, -1))
    attn1 = spread_pair(attn1, attn1_x)
    mlp1 = spread_pair(mlp1, mlp1_x)
    sent_ho, kept_ho = attn(1, pieces, assemble_shifted, (attn1, 0), table1, (SENT, TOK - SENT))
    blocks = ((attn1, 3), (mlp1, 0), (mlp1, 4))
    sent = feed(1, pieces[1:], assemble_sent, finish_sent, shapes[1:], blocks, sent_ho)
    (own,) = feed(1, (pieces[0],), assemble_kept, finish_kept, shapes[:1], blocks, kept_ho)
    return join(own, *exchange(*sent, 1))


def solution(mesh):
    fine = jax.sharding.Mesh(mesh.devices.reshape(SIZES), AXES)
    tokens = P(("img", "row"), ("x", "yh", "c"), None)
    weight = P(None, ("x", "yh", "c"), None)
    in_specs = (tokens, weight, weight, weight, weight, P(), P(), P(), P(), P())

    return jax.shard_map(local, mesh=fine, in_specs=in_specs, out_specs=tokens, check_vma=False)
```

```python
import math

import jax
import jax.numpy as jnp
import numpy as np
from jax import lax
from jax.experimental import pallas as pl
from jax.experimental.pallas import tpu as pltpu
from jax.sharding import PartitionSpec as P


HEADS = 16
WIN = 12
SHIFT = 6
D = 512
FF = 2048
HD = 32
KEYS = WIN * WIN
NWIN = 3
TOK = KEYS * NWIN
LOG2E = math.log2(math.e)
BF = jnp.bfloat16
F32 = jnp.float32
MIB = 1024 * 1024
NT = (((1,), (1,)), ((), ()))
NN = (((1,), (0,)), ((), ()))
AXES = ("row", "x", "yh", "c", "img")
SIZES = (8, 4, 2, 2, 2)


def dot(a, b, dims=NN):
    return lax.dot_general(a, b, dims, preferred_element_type=F32)


def layer_norm(values, gain, shift):
    center = values - jnp.mean(values, -1, keepdims=True)
    spread = jnp.mean(center * center, -1, keepdims=True)
    return center * lax.rsqrt(spread + 1e-05) * gain + shift


def bias_kernel(masked, t_ref, side_ref, out_ref, rows, mask):
    lane = lax.broadcasted_iota(jnp.int32, (HEADS, 128), 1)
    n_off = 2 * WIN - 1
    for cb in range(WIN):
        tiles = [jnp.zeros((HEADS, 128), F32) for _ in range(3)]
        for ro in range(n_off):
            moved = pltpu.roll(t_ref[ro], (ro * WIN - (WIN - 1 - cb)) % 128, 1)
            for tile in range(ro * WIN // 128, (ro * WIN + WIN - 1) // 128 + 1):
                low = ro * WIN - tile * 128
                tiles[tile] = jnp.where((lane >= low) & (lane < low + WIN), moved, tiles[tile])
        for tile in range(3):
            rows[tile, (cb + 4) * HEADS : (cb + 5) * HEADS, :] = tiles[tile] * LOG2E
    if masked:
        last_row = (lax.axis_index("row") == 7).astype(F32)
        col = (lax.axis_index("x") * 2 + lax.axis_index("yh")) * 2 + lax.axis_index("c")
        last_col = (col == 15).astype(F32)
        below = side_ref[0:1, :TOK]
        right = side_ref[1:2, :TOK]
        here = side_ref[2:3, :TOK]
        key_right = (lax.broadcasted_iota(jnp.int32, (WIN, 1), 0) >= SHIFT).astype(F32)
        across = last_col * here * jnp.abs(right - key_right)
        for rb in range(WIN):
            down = last_row * jnp.abs(below - (1.0 if rb >= SHIFT else 0.0))
            mask[rb * WIN : (rb + 1) * WIN, :] = jnp.maximum(across, down) * -1e9
    lane = lax.broadcasted_iota(jnp.int32, (16, 128), 1)
    upper = lax.broadcasted_iota(jnp.int32, (8, 128), 0) < 4

    def one_line(mine, at, t):
        value = None
        for w in range(NWIN):
            for s in range(3):
                low = max(KEYS * w, s * 128 + KEYS * w - at) - t * 128
                high = min(KEYS * (w + 1), (s + 1) * 128 + KEYS * w - at) - t * 128
                if max(low, 0) >= min(high, 128):
                    continue
                moved = pltpu.roll(mine[s], (KEYS * w - at) % 128, 1)
                value = moved if value is None else jnp.where(lane >= low, moved, value)
        return value

    def one_head(h, carry):
        even = [rows[tile, pl.ds(h + 4 * HEADS, 16, stride=HEADS), :] for tile in range(3)]
        odd = [rows[tile, pl.ds(h, 16, stride=HEADS), :] for tile in range(3)]
        for pair_at in range(WIN // 2):
            for t in range(4):
                first = one_line(even, (WIN - 1 - 2 * pair_at) * WIN, t)
                second = one_line(odd, (WIN - 2 - 2 * pair_at) * WIN, t)
                whole = jnp.concatenate(
                    [first[:8], jnp.where(upper, first[8:], second[:8]), second[8:]], axis=0)
                width = min(TOK - t * 128, 128)
                at = slice(pair_at * 24, (pair_at + 1) * 24), slice(t * 128, t * 128 + width)
                whole = whole[:, :width]
                if masked:
                    whole = whole + mask[at[0], at[1]]
                out_ref[h, at[0], at[1]] = whole
        return carry

    lax.fori_loop(0, HEADS, one_head, 0)


def bias_table(t, masked, after=()):
    vm = pl.BlockSpec(memory_space=pltpu.VMEM)
    at = np.arange(512)
    side = np.zeros((8, 512), np.float32)
    side[0] = at % KEYS >= SHIFT * WIN
    side[1] = at % WIN >= SHIFT
    side[2] = (at >= 2 * KEYS) & (at < TOK)

    def body(*refs):
        bias_kernel(masked, refs[0], refs[1], *refs[-3:])

    return pl.pallas_call(
        body,
        out_shape=jax.ShapeDtypeStruct((HEADS, KEYS, TOK), F32),
        in_specs=[vm, vm] + [pl.BlockSpec(memory_space=pl.ANY)] * len(after),
        out_specs=vm,
        scratch_shapes=[pltpu.VMEM((3, 20 * HEADS, 128), F32), pltpu.VMEM((KEYS, TOK), F32)],
        compiler_params=pltpu.CompilerParams(vmem_limit_bytes=8 * MIB),
        name="bias_table",
    )(t, jnp.asarray(side), *after)


def fetch_blocks(refs, tags, first, count, dst, whole):
    core = lax.axis_index("c")
    my_yh = lax.axis_index("yh")
    my_x = lax.axis_index("x")
    for ref, (kind, flip, shift) in zip(refs, tags):
        c = 1 - core if flip else core
        if kind == "all":
            for k, dx in enumerate((0, *X_MOVES)):
                for yh in range(2):
                    col = lax.rem(my_x + 4 - dx, 4) * 4 + yh * 2 + c
                    rows = pl.ds(pl.multiple_of(col * 32, 32), 32)
                    dst[:, rows, :] = ref[k, yh, first : first + count]
            continue
        for i in range(ref.shape[0]):
            if kind == "x":
                col = i * 4 + (1 - my_yh if shift else my_yh) * 2 + c
            else:
                col = lax.rem(my_x + 4 - shift, 4) * 4 + i * 2 + c
            block = ref[i, first : first + count]
            if whole:
                dst[col] = block
            else:
                dst[:, pl.ds(pl.multiple_of(col * 32, 32), 32), :] = block


def one_hot(where_ref, which, start, count):
    i = lax.broadcasted_iota(jnp.int32, (count, TOK), 0) + start
    return (i == where_ref[which : which + 1, :TOK]).astype(F32).astype(BF)


def attn_kernel(n_pieces, layer, tags, assemble, first, *refs):
    n_w = len(tags)
    pieces = refs[:n_pieces]
    wrefs = refs[n_pieces : n_pieces + n_w]
    at = n_pieces + n_w
    where_ref, bq_all, gain_ref, mbias_ref, bt_ref = refs[at : at + 5]
    hos = refs[at + 5 : -6]
    xs, qs, ks, vts, ots, w_ref = refs[-6:]
    bq_ref = bq_all.at[layer : layer + 1]
    fetch_blocks(wrefs, tags, first, 3, w_ref, False)
    assemble(pieces, xs)
    normed = layer_norm(xs[...], gain_ref[layer, 0:1], mbias_ref[layer, 0:1]).astype(BF)
    nw = dot(one_hot(where_ref, 0, 0, TOK), normed).astype(BF)
    scale = LOG2E / math.sqrt(HD)
    for kind in range(2):
        y = dot(nw, w_ref[kind]) + bq_ref[:, kind * D : (kind + 1) * D]
        if kind == 0:
            y = y * scale
        dst = qs if kind == 0 else ks
        for w in range(NWIN):
            rows = slice(w * KEYS, (w + 1) * KEYS)
            for g in range(4):
                tile = y[rows, g * 128 : (g + 1) * 128]
                if w:
                    tile = pltpu.roll(tile, HD * w, 1)
                dst[g, rows, :] = tile.astype(BF)
    v = (dot(nw, w_ref[2]) + bq_ref[:, 2 * D :]).astype(BF)
    eye = (lax.broadcasted_iota(jnp.int32, (128, 128), 0)
           == lax.broadcasted_iota(jnp.int32, (128, 128), 1)).astype(BF)
    for w in range(NWIN):
        for g in range(4):
            vt = dot(eye, v[w * KEYS : (w + 1) * KEYS, g * 128 : (g + 1) * 128], NT).astype(BF)
            for hh in range(4):
                vts[g * 4 + hh, w * HD : (w + 1) * HD, :] = vt[hh * HD : (hh + 1) * HD]
    for h in range(HEADS):
        vts[h, NWIN * HD :, :] = jnp.ones((16, KEYS), BF)
    lane_slot = lax.broadcasted_iota(jnp.int32, (1, 128), 1) // HD
    slot = [(lane_slot == s).astype(F32).astype(BF) for s in range(4)]
    win = lax.broadcasted_iota(jnp.int32, (1, TOK), 1)

    def four_heads(g, carry):
        for hh in range(4):
            h = g * 4 + hh
            kcat = ks[g, 0:KEYS, :] * slot[hh]
            for w in range(1, NWIN):
                kcat = kcat + ks[g, w * KEYS : (w + 1) * KEYS, :] * slot[(hh + w) % 4]
            qbd = jnp.concatenate(
                [qs[g, w * KEYS : (w + 1) * KEYS, :] * slot[(hh + w) % 4] for w in range(NWIN)], axis=0)
            st = dot(kcat, qbd, NT) + bt_ref[h]
            p = jnp.exp2(st - jnp.max(st, axis=0, keepdims=True)).astype(BF)
            o = dot(vts[h], p)
            mine = jnp.where(win < KEYS, o[0:HD], jnp.where(win < 2 * KEYS, o[HD : 2 * HD], o[2 * HD : 3 * HD]))
            ots[h] = (mine * (1.0 / o[3 * HD : 3 * HD + 1])).astype(BF)
        return carry

    lax.fori_loop(0, HEADS // 4, four_heads, 0)
    first_token = 0
    for ho_ref in hos:
        pick = one_hot(where_ref, 1, first_token, ho_ref.shape[0])
        ho_ref[...] = dot(pick, ots[...].reshape(D, TOK), NT).astype(BF)
        first_token += ho_ref.shape[0]


def attention(layer, pieces, assemble, weights, where, counts, bq, gain, mbias, bt):
    (blocks, tags), first = weights
    n, m = len(pieces), len(blocks)
    vm = pl.BlockSpec(memory_space=pltpu.VMEM)
    return pl.pallas_call(
        lambda *refs: attn_kernel(n, layer, tags, assemble, first, *refs),
        out_shape=[jax.ShapeDtypeStruct((count, D), BF) for count in counts],
        in_specs=[vm] * (n + m + 5),
        out_specs=[vm] * len(counts),
        scratch_shapes=[
            pltpu.VMEM((TOK, D), F32),
            pltpu.VMEM((4, TOK, 128), BF),
            pltpu.VMEM((4, TOK, 128), BF),
            pltpu.VMEM((HEADS, NWIN * HD + 16, KEYS), BF),
            pltpu.VMEM((HEADS, HD, TOK), BF),
            pltpu.VMEM((3, D, D), BF),
        ],
        compiler_params=pltpu.CompilerParams(vmem_limit_bytes=20 * MIB),
        cost_estimate=pl.CostEstimate(flops=10_000_000_000, bytes_accessed=8_000_000, transcendentals=0),
        name="attention",
    )(*pieces, *blocks, where, bq, gain, mbias, bt)


def mlp_kernel(n_pieces, layer, tags, firsts, assemble, finish, *refs):
    pieces = refs[:n_pieces]
    ho_ref, bh_all, gain_ref, mbias_ref = refs[n_pieces : n_pieces + 4]
    bh_ref = bh_all.at[layer : layer + 1]
    at = n_pieces + 4
    blocks = []
    for shared, group in tags:
        if shared is not None:
            blocks.append(blocks[shared])
            continue
        blocks.append(refs[at : at + len(group)])
        at += len(group)
    tags = [group for _, group in tags]
    outs = refs[at:-5]
    xs, acc, wp_ref, wh_ref, wo_ref = refs[-5:]
    fetch_blocks(blocks[0], tags[0], firsts[0], 1, wp_ref, False)
    fetch_blocks(blocks[1], tags[1], firsts[1], 4, wh_ref, False)
    fetch_blocks(blocks[2], tags[2], firsts[2], 4, wo_ref, True)
    assemble(pieces, xs)
    mid = xs[...] + (dot(ho_ref[...], wp_ref[0]) + mbias_ref[layer, 2:3])
    xs[...] = mid
    n2 = layer_norm(mid, gain_ref[layer, 1:2], mbias_ref[layer, 1:2]).astype(BF)
    step = 512
    for c in range(FF // step):
        cols = slice(c * step, (c + 1) * step)
        z = dot(n2, wh_ref[c]) + bh_ref[:, cols]
        hid = (0.5 * z * (1.0 + lax.erf(z * math.sqrt(0.5)))).astype(BF)
        part = dot(hid, wo_ref[4 * c : 4 * c + 4].reshape(step, D))
        acc[...] = part if c == 0 else acc[...] + part
    xs[...] = xs[...] + (acc[...] + mbias_ref[layer, 3:4])
    finish(xs, outs)


def mlp(layer, pieces, assemble, finish, outs, weights, ho, bh, gain, mbias):
    tokens = ho.shape[0]
    tags, blocks = [], []
    for i, (group, _) in enumerate(weights):
        same = [j for j in range(i) if weights[j][0] is group]
        tags.append((same[0] if same else None, group[1]))
        blocks += () if same else group[0]
    firsts = [first for _, first in weights]
    n = len(pieces)
    vm = pl.BlockSpec(memory_space=pltpu.VMEM)
    return pl.pallas_call(
        lambda *refs: mlp_kernel(n, layer, tags, firsts, assemble, finish, *refs),
        out_shape=outs,
        in_specs=[vm] * (n + 4 + len(blocks)),
        out_specs=[vm] * len(outs),
        scratch_shapes=[
            pltpu.VMEM((tokens, D), F32),
            pltpu.VMEM((tokens, D), F32),
            pltpu.VMEM((1, D, D), BF),
            pltpu.VMEM((4, D, D), BF),
            pltpu.VMEM((16, 4, 32, D), BF),
        ],
        compiler_params=pltpu.CompilerParams(vmem_limit_bytes=20 * MIB),
        cost_estimate=pl.CostEstimate(flops=10_000_000_000, bytes_accessed=8_000_000, transcendentals=0),
        name="mlp",
    )(*pieces, ho, bh, gain, mbias, *blocks)


ROWS = WIN
COLS = WIN * NWIN
KEEP = COLS - SHIFT


def assemble_plain(pieces, xs):
    for r in range(ROWS):
        xs[r * COLS : (r + 1) * COLS, :] = pieces[0][r].astype(F32)


SENT = SHIFT * (COLS + SHIFT)


def assemble_sent(pieces, xs):
    right, below, corner = pieces
    for r in range(SHIFT):
        xs[r * COLS : r * COLS + KEEP, :] = below[r].astype(F32)
        xs[r * COLS + KEEP : (r + 1) * COLS, :] = corner[r].astype(F32)
        at = SHIFT * (COLS + r)
        xs[at : at + SHIFT, :] = right[r].astype(F32)


def assemble_kept(pieces, xs, base=0):
    for r in range(SHIFT):
        xs[base + r * KEEP : base + (r + 1) * KEEP, :] = pieces[0][r].astype(F32)


def assemble_shifted(pieces, xs):
    assemble_sent(pieces[1:], xs)
    assemble_kept(pieces, xs, SENT)


def finish_first(xs, outs):
    own, right, below, corner = outs
    for r in range(SHIFT):
        top = xs[r * COLS : (r + 1) * COLS, :].astype(BF)
        below[r] = top[SHIFT:]
        corner[r] = top[:SHIFT]
        low = xs[(r + SHIFT) * COLS : (r + SHIFT + 1) * COLS, :].astype(BF)
        own[r] = low[SHIFT:]
        right[r] = low[:SHIFT]


def finish_sent(xs, outs):
    right, below, corner = outs
    for r in range(SHIFT):
        low = xs[r * COLS : (r + 1) * COLS, :].astype(BF)
        below[r] = low[:KEEP]
        corner[r] = low[KEEP:]
        at = SHIFT * (COLS + r)
        right[r] = xs[at : at + SHIFT, :].astype(BF)


def finish_kept(xs, outs):
    for r in range(SHIFT):
        outs[0][r] = xs[r * KEEP : (r + 1) * KEEP, :].astype(BF)


def join_kernel(own, right, below, corner, out):
    for r in range(SHIFT):
        out[r] = jnp.concatenate([corner[r].astype(F32), below[r].astype(F32)], axis=0).astype(BF)
        out[r + SHIFT] = jnp.concatenate([right[r].astype(F32), own[r].astype(F32)], axis=0).astype(BF)


def join(*pieces):
    return pl.pallas_call(
        join_kernel,
        out_shape=jax.ShapeDtypeStruct((ROWS, COLS, D), BF),
        compiler_params=pltpu.CompilerParams(vmem_limit_bytes=4 * MIB),
        name="join",
    )(*pieces)


def part_shapes():
    return (
        jax.ShapeDtypeStruct((SHIFT, KEEP, D), BF),
        jax.ShapeDtypeStruct((SHIFT, SHIFT, D), BF),
        jax.ShapeDtypeStruct((SHIFT, KEEP, D), BF),
        jax.ShapeDtypeStruct((SHIFT, SHIFT, D), BF),
    )


def places(shifted):
    table = np.full((8, 512), -1, np.int32)
    for r in range(ROWS):
        for c in range(COLS):
            if not shifted:
                at = r * COLS + c
            elif r >= SHIFT:
                at = (r - SHIFT) * COLS + c
            elif c >= KEEP:
                at = SHIFT * (COLS + r) + c - KEEP
            else:
                at = SENT + r * KEEP + c
            place = (c // WIN) * KEYS + r * WIN + c % WIN
            table[0, at] = place
            table[1, place] = at
    return jnp.asarray(table)


def bias_rows(table):
    return jnp.pad(table.transpose(0, 2, 1, 3), ((0, 0), (0, 0), (0, 0), (0, 128 - (2 * WIN - 1))))


def send(block, where):
    pairs = []
    for at in np.ndindex(*SIZES):
        row, x, yh, c, img = at
        row2, x2, y2, c2 = where(row, x, yh * 2 + img, c)
        to = (row2 % 8, x2 % 4, y2 % 4 // 2, c2, y2 % 2)
        pairs.append((int(np.ravel_multi_index(at, SIZES)), int(np.ravel_multi_index(to, SIZES))))
    return lax.ppermute(block, AXES, pairs)


def shift_tokens(block, rows, cols):
    def where(row, x, y, c):
        col = (x * 4 + y // 2 * 2 + c + cols) % 16
        return row + rows, col // 4, col // 2 % 2 * 2 + y % 2, col % 2

    return send(block, where)


def swap_cores(block):
    return send(block, lambda row, x, y, c: (row, x, y, 1 - c))


def chunk_kernel(picks, n_in, *refs):
    arrays, outs, sem = refs[:n_in], refs[n_in:-1], refs[-1]
    copies = []
    for g, (out, group) in enumerate(zip(outs, picks)):
        at = 0
        for layer, which in group:
            ref = arrays[which]
            for rows in range(ref.shape[1] // 32):
                for lanes in range(ref.shape[2] // D):
                    part = ref.at[layer, pl.ds(rows * 32, 32), pl.ds(lanes * D, D)]
                    copies.append(pltpu.make_async_copy(part, out.at[at], sem.at[g, at]))
                    at += 1
    for copy in copies:
        copy.start()
    for copy in copies:
        copy.wait()


def chunks(picks, weights):
    sizes = [w.shape[1] // 32 * (w.shape[2] // D) for w in weights]
    counts = [sum(sizes[which] for _, which in group) for group in picks]
    return pl.pallas_call(
        lambda *refs: chunk_kernel(picks, len(weights), *refs),
        out_shape=[jax.ShapeDtypeStruct((n, 32, D), BF) for n in counts],
        in_specs=[pl.BlockSpec(memory_space=pltpu.HBM)] * len(weights),
        out_specs=[pl.BlockSpec(memory_space=pltpu.VMEM)] * len(counts),
        scratch_shapes=[pltpu.SemaphoreType.DMA((len(counts), max(counts)))],
        compiler_params=pltpu.CompilerParams(vmem_limit_bytes=8 * MIB),
        name="chunks",
    )(*weights)


X_MOVES = (1, 3, 2)


def join_x_kernel(n_after, own, *refs):
    came, out = refs[:3], refs[3 + n_after]
    x = lax.axis_index("x")
    for k, ref in enumerate((own, *came)):
        out[x if k == 0 else lax.rem(x + 4 - X_MOVES[k - 1], 4)] = ref[...]


def join_x(own, came, after):
    vm = pl.BlockSpec(memory_space=pltpu.VMEM)
    return pl.pallas_call(
        lambda *refs: join_x_kernel(len(after), *refs),
        out_shape=jax.ShapeDtypeStruct((4, *own.shape), BF),
        in_specs=[vm] * 4 + [pl.BlockSpec(memory_space=pl.ANY)] * len(after),
        out_specs=vm,
        compiler_params=pltpu.CompilerParams(vmem_limit_bytes=8 * MIB),
        name="join_x",
    )(own, *came, *after)


def pair_kernel(cuts, own, other, *refs):
    yh = lax.axis_index("yh")
    for (lo, hi), out in zip(cuts, refs[-len(cuts) :]):
        out[yh] = own[lo:hi]
        out[1 - yh] = other[lo:hi]


def pair(own, other, cuts, after):
    vm = pl.BlockSpec(memory_space=pltpu.VMEM)
    return pl.pallas_call(
        lambda *refs: pair_kernel(cuts, *refs),
        out_shape=[jax.ShapeDtypeStruct((2, hi - lo, 32, D), BF) for lo, hi in cuts],
        in_specs=[vm] * 2 + [pl.BlockSpec(memory_space=pl.ANY)] * len(after),
        out_specs=[vm] * len(cuts),
        compiler_params=pltpu.CompilerParams(vmem_limit_bytes=8 * MIB),
        name="pair",
    )(own, other, *after)


def stack_kernel(*refs):
    for k, ref in enumerate(refs[:-1]):
        refs[-1][k] = ref[...]


def spread_stack(both, came):
    mine = pl.pallas_call(
        stack_kernel,
        out_shape=jax.ShapeDtypeStruct((4, *both.shape), BF),
        compiler_params=pltpu.CompilerParams(vmem_limit_bytes=8 * MIB),
        name="stack",
    )(both, *came)
    return (mine, swap_cores(mine)), (("all", 0, 0), ("all", 1, 0))


def along_x(block):
    return [send(block, lambda row, x, y, c, dx=dx: (row, x + dx, y, c)) for dx in X_MOVES]


def across_y(block):
    return send(block, lambda row, x, y, c: (row, x, 3 - y, c))


def both_cores(mine, other):
    blocks = (mine, swap_cores(mine), other, swap_cores(other))
    return blocks, (("x", 0, 0), ("x", 1, 0), ("x", 0, 1), ("x", 1, 1))


def spread_pair(both, came):
    blocks, tags = [], []
    for dx, block in zip((0, *X_MOVES), (both, *came)):
        blocks += [block, swap_cores(block)]
        tags += [("yh", 0, dx), ("yh", 1, dx)]
    return blocks, tags


def local(
    tokens,
    qkv_weight,
    proj_weight,
    hidden_weight,
    output_weight,
    norm_gain,
    model_bias,
    qkv_bias,
    hidden_bias,
    position_bias,
):
    weights = (qkv_weight, proj_weight, hidden_weight, output_weight)
    (first,) = chunks((((0, 0),),), (qkv_weight,))
    rest, pairs, mlp1 = chunks(
        (((0, 1), (0, 2)), ((0, 3), (1, 0), (1, 1)), ((1, 2), (1, 3))), weights
    )
    rows = bias_rows(position_bias)
    first_y = across_y(first)
    rest_x = along_x(rest)
    pairs_y = across_y(pairs)
    (first,) = pair(first, first_y, ((0, 3),), ())
    first_x = along_x(first)
    qkv0 = spread_stack(first, first_x)
    table0 = bias_table(rows[0], False, (first,))
    rest_mine = join_x(rest, rest_x, (table0,))
    rest_other = across_y(rest_mine)
    mlp1_x = along_x(mlp1)
    down0, attn1 = pair(pairs, pairs_y, ((0, 4), (4, 8)), (rest_mine,))
    down0_x = along_x(down0)

    def attn(k, pieces, assemble, blocks, table, counts):
        params = (qkv_bias, norm_gain, model_bias, table)
        return attention(k, pieces, assemble, blocks, places(k), counts, *params)

    def feed(k, pieces, assemble, finish, outs, blocks, ho):
        return mlp(k, pieces, assemble, finish, outs, blocks, ho, hidden_bias, norm_gain, model_bias)

    def exchange(right, below, corner, way):
        corner = shift_tokens(corner, way, way)
        right = shift_tokens(right, 0, way)
        below = shift_tokens(below, way, 0)
        return right, below, corner

    (ho,) = attn(0, (tokens,), assemble_plain, (qkv0, 0), table0, (TOK,))
    attn1, ho = lax.optimization_barrier((attn1, ho))
    attn1_x = along_x(attn1)
    mlp1_mine = join_x(mlp1, mlp1_x, (ho,))
    mlp1_other = across_y(mlp1_mine)
    rest0 = both_cores(rest_mine, rest_other)
    down0 = spread_pair(down0, down0_x)
    shapes = part_shapes()
    own, *halo = feed(
        0, (tokens,), assemble_plain, finish_first, shapes, ((rest0, 0), (rest0, 1), (down0, 0)), ho
    )
    table1 = bias_table(rows[1], True, tuple(halo))
    pieces = (own, *exchange(*halo, -1))
    attn1 = spread_stack(attn1, attn1_x)
    mlp1 = both_cores(mlp1_mine, mlp1_other)
    sent_ho, kept_ho = attn(1, pieces, assemble_shifted, (attn1, 0), table1, (SENT, TOK - SENT))
    blocks = ((attn1, 3), (mlp1, 0), (mlp1, 4))
    sent = feed(1, pieces[1:], assemble_sent, finish_sent, shapes[1:], blocks, sent_ho)
    (own,) = feed(1, (pieces[0],), assemble_kept, finish_kept, shapes[:1], blocks, kept_ho)
    return join(own, *exchange(*sent, 1))


def solution(mesh):
    fine = jax.sharding.Mesh(mesh.devices.reshape(SIZES), AXES)
    tokens = P(("img", "row"), ("x", "yh", "c"), None)
    weight = P(None, ("x", "yh", "c"), None)
    in_specs = (tokens, weight, weight, weight, weight, P(), P(), P(), P(), P())

    return jax.shard_map(local, mesh=fine, in_specs=in_specs, out_specs=tokens, check_vma=False)
```
